256 devices in a mesh: tp: 4 (over x), fsdp: 64 (over z, y, core).
Axes of the slice: x: 4, y: 4, z: 8, core: 2. Of those that a mesh axis runs over, the one named last changes fastest.
Arguments:
- patches: bfloat16 [4096, 49, 3072], P('fsdp')
- labels: int32 [4096], P('fsdp')
- w_stem: float32 [3072, 512], P('fsdp', 'tp')
- b_stem: float32 [512], P(('tp', 'fsdp'))
- ln1_g: float32 [2, 512], P(None, ('tp', 'fsdp'))
- ln1_b: float32 [2, 512], P(None, ('tp', 'fsdp'))
- w_tok1: float32 [2, 49, 256], P(None, None, 'fsdp')
- b_tok1: float32 [2, 256], P(None, 'fsdp')
- w_tok2: float32 [2, 256, 49], P(None, 'fsdp')
- ln2_g: float32 [2, 512], P(None, ('tp', 'fsdp'))
- ln2_b: float32 [2, 512], P(None, ('tp', 'fsdp'))
- w_ch1: float32 [2, 512, 2048], P(None, 'fsdp', 'tp')
- b_ch1: float32 [2, 2048], P(None, ('tp', 'fsdp'))
- w_ch2: float32 [2, 2048, 512], P(None, ('tp', 'fsdp'))
- b_ch2: float32 [2, 512], P(None, ('tp', 'fsdp'))
- lnf_g: float32 [512], P(('tp', 'fsdp'))
- lnf_b: float32 [512], P(('tp', 'fsdp'))
- w_head: float32 [512, 1000], P('fsdp', 'tp')
- b_head: float32 [1000], P('tp')
Outputs:
- output 1: float32 [], replicated
- output 2: float32 [3072, 512], P('fsdp', 'tp')
- output 3: float32 [512], P(('tp', 'fsdp'))
- output 4: float32 [2, 512], P(None, ('tp', 'fsdp'))
- output 5: float32 [2, 512], P(None, ('tp', 'fsdp'))
- output 6: float32 [2, 49, 256], P(None, None, 'fsdp')
- output 7: float32 [2, 256], P(None, 'fsdp')
- output 8: float32 [2, 256, 49], P(None, 'fsdp')
- output 9: float32 [2, 512], P(None, ('tp', 'fsdp'))
- output 10: float32 [2, 512], P(None, ('tp', 'fsdp'))
- output 11: float32 [2, 512, 2048], P(None, 'fsdp', 'tp')
- output 12: float32 [2, 2048], P(None, ('tp', 'fsdp'))
- output 13: float32 [2, 2048, 512], P(None, ('tp', 'fsdp'))
- output 14: float32 [2, 512], P(None, ('tp', 'fsdp'))
- output 15: float32 [512], P(('tp', 'fsdp'))
- output 16: float32 [512], P(('tp', 'fsdp'))
- output 17: float32 [512, 1000], P('fsdp', 'tp')
- output 18: float32 [1000], P('tp')
All inputs are finite; a program needn't handle non-finite values.
Results may differ from the reference program's by a relative error of at most 0.0136364.
Values are sent between devices in bfloat16 or wider.
A program may use at most 768 MiB of HBM per device.

```python
import jax
import jax.numpy as jnp
from jax import lax

PATCH_SIDE = 32
TOKENS = 49
CHANNELS = 512
TOKEN_HIDDEN = 256
CHANNEL_HIDDEN = 2048
CLASSES = 1000
LAYERS = 2
IMAGES = 4096
BLOCKS = 64

PATCH_DIM = 3 * PATCH_SIDE * PATCH_SIDE
PER_BLOCK = IMAGES // BLOCKS
EPS = 1e-6
LAYER_NAMES = ('ln1_g', 'ln1_b', 'w_tok1', 'b_tok1', 'w_tok2', 'ln2_g', 'ln2_b', 'w_ch1', 'b_ch1', 'w_ch2', 'b_ch2')


def setup_inputs(seed: int = 0) -> dict:
    key_list = jax.random.split(jax.random.key(seed), 20)

    def normal(index, shape, scale):
        return scale * jax.random.normal(key_list[index], shape, jnp.float32)

    chan_shape = (LAYERS, CHANNELS)
    return {
        'patches': normal(0, (IMAGES, TOKENS, PATCH_DIM), 1.0).astype(jnp.bfloat16),
        'labels': jax.random.randint(key_list[1], (IMAGES,), 0, CLASSES, jnp.int32),
        'w_stem': normal(2, (PATCH_DIM, CHANNELS), PATCH_DIM ** -0.5),
        'b_stem': normal(3, (CHANNELS,), 0.5),
        'ln1_g': 1.0 + normal(4, chan_shape, 0.3),
        'ln1_b': normal(5, chan_shape, 0.3),
        'w_tok1': normal(6, (LAYERS, TOKENS, TOKEN_HIDDEN), TOKENS ** -0.5),
        'b_tok1': normal(7, (LAYERS, TOKEN_HIDDEN), 0.3),
        'w_tok2': normal(8, (LAYERS, TOKEN_HIDDEN, TOKENS), TOKEN_HIDDEN ** -0.5),
        'ln2_g': 1.0 + normal(9, chan_shape, 0.3),
        'ln2_b': normal(10, chan_shape, 0.3),
        'w_ch1': normal(11, (LAYERS, CHANNELS, CHANNEL_HIDDEN), CHANNELS ** -0.5),
        'b_ch1': normal(12, (LAYERS, CHANNEL_HIDDEN), 0.3),
        'w_ch2': normal(13, (LAYERS, CHANNEL_HIDDEN, CHANNELS), CHANNEL_HIDDEN ** -0.5),
        'b_ch2': normal(14, chan_shape, 0.3),
        'lnf_g': 1.0 + normal(15, (CHANNELS,), 0.3),
        'lnf_b': normal(16, (CHANNELS,), 0.3),
        'w_head': normal(17, (CHANNELS, CLASSES), CHANNELS ** -0.5),
        'b_head': normal(18, (CLASSES,), 0.5),
    }


def as_matmul(values):
    return values.astype(jnp.bfloat16).astype(jnp.float32)


def layer_norm(values, gain, shift):
    mean_val = jnp.mean(values, axis=-1, keepdims=True)
    centered = values - mean_val
    var_val = jnp.mean(centered * centered, axis=-1, keepdims=True)
    return centered * lax.rsqrt(var_val + EPS) * gain + shift


def mixer_layer(resid, layer):
    normed = as_matmul(layer_norm(resid, layer['ln1_g'], layer['ln1_b']))
    hidden = jnp.einsum('bsc,sj->bcj', normed, as_matmul(layer['w_tok1'])) + layer['b_tok1']
    mixed = jnp.einsum('bcj,js->bsc', as_matmul(jax.nn.gelu(hidden)), as_matmul(layer['w_tok2']))
    resid = resid + mixed
    normed = as_matmul(layer_norm(resid, layer['ln2_g'], layer['ln2_b']))
    hidden = jnp.einsum('bsc,cd->bsd', normed, as_matmul(layer['w_ch1'])) + layer['b_ch1']
    out_val = jnp.einsum('bsd,dc->bsc', as_matmul(jax.nn.gelu(hidden)), as_matmul(layer['w_ch2']))
    return resid + out_val + layer['b_ch2'], None


def block_loss(weights, patch_blk, label_blk):
    resid = jnp.einsum('bsp,pc->bsc', patch_blk.astype(jnp.float32), as_matmul(weights['w_stem'])) + weights['b_stem']
    layer_weights = {name: weights[name] for name in LAYER_NAMES}
    resid = lax.scan(mixer_layer, resid, layer_weights)[0]
    pooled = jnp.mean(resid, axis=1)
    normed = as_matmul(layer_norm(pooled, weights['lnf_g'], weights['lnf_b']))
    logits = jnp.einsum('bc,ck->bk', normed, as_matmul(weights['w_head'])) + weights['b_head']
    log_norm = jax.nn.logsumexp(logits, axis=-1)
    class_ids = jnp.arange(CLASSES, dtype=jnp.int32)
    picked = jnp.sum(jnp.where(class_ids[None, :] == label_blk[:, None], logits, 0.0), axis=-1)
    return jnp.sum(log_norm - picked)


def reference(patches, labels, w_stem, b_stem, ln1_g, ln1_b, w_tok1, b_tok1, w_tok2,
              ln2_g, ln2_b, w_ch1, b_ch1, w_ch2, b_ch2, lnf_g, lnf_b, w_head, b_head):
    weights = dict(w_stem=w_stem, b_stem=b_stem, ln1_g=ln1_g, ln1_b=ln1_b, w_tok1=w_tok1,
                   b_tok1=b_tok1, w_tok2=w_tok2, ln2_g=ln2_g, ln2_b=ln2_b, w_ch1=w_ch1,
                   b_ch1=b_ch1, w_ch2=w_ch2, b_ch2=b_ch2, lnf_g=lnf_g, lnf_b=lnf_b,
                   w_head=w_head, b_head=b_head)
    patch_blocks = patches.reshape(BLOCKS, PER_BLOCK, TOKENS, PATCH_DIM)
    label_blocks = labels.reshape(BLOCKS, PER_BLOCK)
    loss_grad = jax.value_and_grad(block_loss)

    def accumulate(carry, block):
        loss_sum, grad_sum = carry
        value, grads = loss_grad(weights, block[0], block[1])
        return (loss_sum + value, jax.tree.map(jnp.add, grad_sum, grads)), None

    start_carry = (jnp.zeros((), jnp.float32), jax.tree.map(jnp.zeros_like, weights))
    loss_sum, grad_sum = lax.scan(accumulate, start_carry, (patch_blocks, label_blocks))[0]
    scale = 1.0 / IMAGES
    return (loss_sum * scale, grad_sum['w_stem'] * scale, grad_sum['b_stem'] * scale,
            grad_sum['ln1_g'] * scale, grad_sum['ln1_b'] * scale, grad_sum['w_tok1'] * scale,
            grad_sum['b_tok1'] * scale, grad_sum['w_tok2'] * scale, grad_sum['ln2_g'] * scale,
            grad_sum['ln2_b'] * scale, grad_sum['w_ch1'] * scale, grad_sum['b_ch1'] * scale,
            grad_sum['w_ch2'] * scale, grad_sum['b_ch2'] * scale, grad_sum['lnf_g'] * scale,
            grad_sum['lnf_b'] * scale, grad_sum['w_head'] * scale, grad_sum['b_head'] * scale)
```

```python
import functools
import jax
import jax.numpy as jnp
from jax import lax
from jax.experimental import pallas as pl
from jax.experimental.pallas import tpu as pltpu
from jax.sharding import PartitionSpec as P

MESH = pl.DeviceIdType.MESH
SIZE = {'x': 4, 'y': 4, 'z': 8, 'c': 2}


class Net:
    def __init__(self, send_sems, recv_sems):
        self.send_sems, self.recv_sems, self.count, self.sent = send_sems, recv_sems, 0, []
        fsdp = lax.axis_index('fsdp')
        self.me = {'x': lax.axis_index('tp'), 'z': fsdp // 8, 'y': (fsdp // 2) % 4, 'c': fsdp % 2}

    def at(self, axis, offset):
        return lax.rem(self.me[axis] + (offset % SIZE[axis]), SIZE[axis])

    def device(self, axis, offset):
        pos = dict(self.me)
        pos[axis] = self.at(axis, offset)
        if axis == 'x':
            return {'tp': pos['x']}
        return {'fsdp': (pos['z'] * 4 + pos['y']) * 2 + pos['c']}

    def barrier(self):
        sem = pltpu.get_barrier_semaphore()
        total = 0
        for axis, size in SIZE.items():
            for offset in range(1, size):
                pl.semaphore_signal(sem, 1, device_id=self.device(axis, offset), device_id_type=MESH)
                total += 1
        pl.semaphore_wait(sem, total)

    def send(self, src, dst, axis, offset):
        i = self.count
        self.count += 1
        copy = pltpu.make_async_remote_copy(src_ref=src, dst_ref=dst, send_sem=self.send_sems.at[i], recv_sem=self.recv_sems.at[i],
                                            device_id=self.device(axis, offset), device_id_type=MESH)
        copy.start()
        self.sent.append(copy)
        return copy

    def finish(self):
        for copy in self.sent:
            copy.wait_send()


def region(tensor, **pos):
    ref, width = tensor
    rows = [pos.get(axis, slice(None)) for axis in 'zyc']
    if width is None:
        return ref.at[tuple([pos.get('x', slice(None))] + rows)]
    cols = slice(None)
    if 'x' in pos:
        cols = pl.ds(pl.multiple_of(pos['x'] * width, width), width)
    return ref.at[tuple(rows + [slice(None), cols])]


HALF = {'x': 'z', 'y': 'z', 'z': 'y'}


def half(axis, which):
    other = HALF[axis]
    n = SIZE[other] // 2
    return {other: pl.ds(which * n, n)}


class Gather:
    def __init__(self, net, tensors, first, middle, last):
        self.net, self.tensors, self.order = net, tensors, (first, middle, last)
        self.core = []

    def direct(self, axis, fixed):
        net, copies = self.net, []
        for t in self.tensors:
            blk = region(t, **{a: net.me[a] for a in fixed})
            for offset in range(1, SIZE[axis]):
                copies.append(net.send(blk, blk, axis, offset))
        return copies

    def phase1(self):
        self.recv = self.direct(self.order[0], 'zycx')

    def arrived(self):
        for copy in self.recv:
            copy.wait_recv()
        self.recv = []

    def phase2(self):
        self.recv = self.direct(self.order[1], [a for a in 'zycx' if a != self.order[0]])

    def to_core(self, **pos):
        net = self.net
        for t in self.tensors:
            blk = region(t, c=net.me['c'], **pos)
            self.core.append(net.send(blk, blk, 'c', 1))

    def ring(self, step):
        net, axis = self.net, self.order[2]
        n = SIZE[axis]
        for sign in (1, -1):
            pos = {axis: net.at(axis, -sign * (step - 1))}
            if step == n // 2:
                pos.update(half(axis, (1 - sign) // 2))
            for t in self.tensors:
                blk = region(t, c=net.me['c'], **pos)
                self.recv.append(net.send(blk, blk, axis, sign))

    def ring_arrived(self, step):
        net, axis = self.net, self.order[2]
        self.arrived()
        if step == 0:
            self.to_core(**{axis: net.me[axis]})
        elif step == SIZE[axis] // 2:
            self.to_core(**{axis: net.at(axis, step)})
        else:
            for sign in (1, -1):
                self.to_core(**{axis: net.at(axis, -sign * step)})

    def core_arrived(self):
        for copy in self.core:
            copy.wait_recv()


def gather_kernel(stem_p, head_p, ch1_p, ch2_p, small_p, stem_o, head_o, c10_o, c11_o, c20_o, c21_o, small_o, bias_o,
                  stem, head, c10, c11, c20, c21, slots, small, merged_bias, send_sems, recv_sems, local_sems, out_sems):
    net = Net(send_sems, recv_sems)
    me = net.me
    tens = {'stem': (stem, 128), 'head': (head, 256), 'c10': (c10, 512), 'c11': (c11, 512), 'c20': (c20, None), 'c21': (c21, None)}
    pieces = (('stem', stem_p), ('head', head_p), ('c10', ch1_p.at[0]), ('c11', ch1_p.at[1]), ('c20', ch2_p.at[0]), ('c21', ch2_p.at[1]))
    loads = [pltpu.make_async_copy(src, region(tens[name], **me), local_sems.at[i]) for i, (name, src) in enumerate(pieces)]
    loads.append(pltpu.make_async_copy(small_p, slots.at[me['x']], local_sems.at[len(pieces)]))
    for copy in loads:
        copy.start()
    net.barrier()
    for copy in loads:
        copy.wait()
    tiny = [net.send(slots.at[me['x']], slots.at[me['x']], 'x', offset) for offset in range(1, 4)]
    a = Gather(net, [tens['stem'], tens['head']], 'x', 'y', 'z')
    b = Gather(net, [tens['c10'], tens['c20']], 'y', 'z', 'x')
    c = Gather(net, [tens['c11'], tens['c21']], 'z', 'x', 'y')
    for g in (a, b, c):
        g.phase1()
    for copy in tiny:
        copy.wait_recv()
    merged = slots[0] + slots[1] + slots[2] + slots[3]
    small[me['z'], me['y'], me['c']] = merged[0:8]
    merged_bias[...] = merged[8:16]
    for g in (a, b, c):
        g.arrived()
        g.phase2()
    mine = small.at[me['z'], me['y'], me['c']]
    tiny = [net.send(mine, mine, 'y', offset) for offset in range(1, 4)]
    a.ring_arrived(0)
    a.ring(1)
    for copy in tiny:
        copy.wait_recv()
    mine = small.at[me['z'], :, me['c']]
    tiny = [net.send(mine, mine, 'z', offset) for offset in range(1, 8)]
    for g in (c, b):
        g.ring_arrived(0)
        g.ring(1)
    for copy in tiny:
        copy.wait_recv()
    mine = small.at[:, :, me['c']]
    tiny = [net.send(mine, mine, 'c', 1)]
    a.ring_arrived(1)
    a.ring(2)
    a.ring_arrived(2)
    a.ring(3)
    for g in (b, c):
        g.ring_arrived(1)
        g.ring(2)
    a.ring_arrived(3)
    a.ring(4)
    for g in (b, c, a):
        g.ring_arrived(SIZE[g.order[2]] // 2)
    outs = []

    def put(src, dst):
        copy = pltpu.make_async_copy(src, dst, out_sems.at[len(outs)])
        copy.start()
        outs.append(copy)

    for copy in tiny:
        copy.wait_recv()
    put(small, small_o)
    put(merged_bias, bias_o)
    b.core_arrived()
    put(c10, c10_o)
    put(c20, c20_o)
    c.core_arrived()
    put(c11, c11_o)
    put(c21, c21_o)
    a.core_arrived()
    put(stem, stem_o)
    put(head, head_o)
    net.finish()
    for copy in outs:
        copy.wait()


def gather_all(stem_p, head_p, ch1_p, ch2_p, small_p):
    bf = jnp.bfloat16
    shapes = [((8, 4, 2, 48, 512), bf), ((8, 4, 2, 8, 1024), bf), ((8, 4, 2, 8, 2048), bf), ((8, 4, 2, 8, 2048), bf),
              ((4, 8, 4, 2, 8, 512), bf), ((4, 8, 4, 2, 8, 512), bf)]
    outs = shapes + [((8, 4, 2, 8, 128), jnp.float32), ((8, 128), jnp.float32)]
    hbm = pl.BlockSpec(memory_space=pl.ANY)
    return pl.pallas_call(
        gather_kernel, out_shape=[jax.ShapeDtypeStruct(s, d) for s, d in outs], in_specs=[hbm] * 5, out_specs=[hbm] * 8,
        scratch_shapes=[pltpu.VMEM(s, d) for s, d in shapes] + [pltpu.VMEM((4, 16, 128), jnp.float32),
                        pltpu.VMEM((8, 4, 2, 8, 128), jnp.float32), pltpu.VMEM((8, 128), jnp.float32), pltpu.SemaphoreType.DMA((160,)), pltpu.SemaphoreType.DMA((160,)),
                        pltpu.SemaphoreType.DMA((7,)), pltpu.SemaphoreType.DMA((8,))],
        compiler_params=pltpu.CompilerParams(collective_id=0, has_side_effects=True, vmem_limit_bytes=48 << 20),
        name='gather_weights')(stem_p, head_p, ch1_p, ch2_p, small_p)


def part(tensor, ref, **pos):
    rows = [pos.get(axis, slice(None)) for axis in tensor['rows']]
    width = tensor['width']
    if width is None:
        return ref.at[tuple([pos.get('x', slice(None))] + rows)]
    cols = slice(None)
    if 'x' in pos:
        cols = pl.ds(pl.multiple_of(pos['x'] * width, width), width)
    return ref.at[tuple(rows + [slice(None), cols])]


def accumulate(dst, srcs):
    lead = dst.shape[:-2]
    total = 1
    for n in lead:
        total *= n

    def body(i, carry):
        idx = []
        for n in reversed(lead):
            idx.append(lax.rem(i, n))
            i = i // n
        idx = tuple(reversed(idx))
        value = dst[idx]
        for src in srcs:
            value = value + src[idx]
        dst[idx] = value
        return carry

    if total == 1:
        idx = (0,) * len(lead)
        value = dst[idx] if lead else dst[...]
        for src in srcs:
            value = value + (src[idx] if lead else src[...])
        if lead:
            dst[idx] = value
        else:
            dst[...] = value
    else:
        lax.fori_loop(0, total, body, 0)


class Reduce:
    def __init__(self, net, tensors, first, middle, last, load_sems):
        self.net, self.tensors, self.order, self.load_sems = net, tensors, (first, middle, last), load_sems
        self.loads, self.recv, self.ready = {}, {}, set()

    def targets(self):
        n = SIZE[self.order[0]]
        order = [n // 2]
        for d in range(n // 2 - 1, 0, -1):
            order += [d, n - d]
        return order + [0]

    def start(self, i):
        net, axis = self.net, self.order[0]
        off = self.targets()[i]
        self.loads[off] = []
        for k, t in enumerate(self.tensors):
            pos = {axis: net.at(axis, off)}
            full = dict(t, rows='zyc')
            src = part(full, t['grad'], c=net.me['c'], **pos)
            load = pltpu.make_async_copy(src, part(t, t['sum'], **pos), self.load_sems.at[i * len(self.tensors) + k])
            load.start()
            away = part(full, t['grad'], c=1 - net.me['c'], **pos)
            self.loads[off].append((load, net.send(away, part(t, t['peer'], **pos), 'c', 1)))

    def prepare(self, off):
        net, axis = self.net, self.order[0]
        off = off % SIZE[axis]
        if off in self.ready:
            return
        self.ready.add(off)
        for t, (load, peer) in zip(self.tensors, self.loads[off]):
            load.wait()
            peer.wait_recv()
            pos = {axis: net.at(axis, off)}
            accumulate(part(t, t['sum'], **pos), [part(t, t['peer'], **pos)])

    def ring(self, step):
        net, axis = self.net, self.order[0]
        n = SIZE[axis]
        off = n // 2 - step + 1
        for sign in (1, -1):
            self.prepare(sign * off)
        copies = []
        for which, sign in enumerate((1, -1)):
            pos = {axis: net.at(axis, sign * off)}
            cut = dict(pos, **half(axis, which))
            for k, t in enumerate(self.tensors):
                if step > 1:
                    self.recv[sign, k].wait_recv()
                    slot = t['ring'][which][step - 2]
                    accumulate(part(t, t['sum'], **(cut if step == 2 else pos)), [slot])
            if step <= n // 2:
                for k, t in enumerate(self.tensors):
                    src = part(t, t['sum'], **(cut if step == 1 else pos))
                    copies.append(((sign, k), net.send(src, t['ring'][which][step - 1], axis, sign)))
        self.recv = dict(copies)

    def direct(self, phase):
        net, axis = self.net, self.order[phase]
        fixed = {a: net.me[a] for a in self.order[:phase]}
        self.recv = []
        for t in self.tensors:
            for offset in range(1, SIZE[axis]):
                src = part(t, t['sum'], **fixed, **{axis: net.at(axis, offset)})
                self.recv.append(net.send(src, t['slots'][phase - 1].at[offset - 1], axis, offset))

    def direct_done(self, phase):
        net, axis = self.net, self.order[phase]
        fixed = {a: net.me[a] for a in self.order[:phase + 1]}
        for copy in self.recv:
            copy.wait_recv()
        for t in self.tensors:
            accumulate(part(t, t['sum'], **fixed), [t['slots'][phase - 1].at[i] for i in range(SIZE[axis] - 1)])


REDUCED = (('stem', 0, 48, 128), ('head', 0, 8, 256), ('c10', 1, 8, 512), ('c20', 1, 8, None), ('c11', 2, 8, 512), ('c21', 2, 8, None))
ORDERS = (('z', 'y', 'x'), ('x', 'z', 'y'), ('y', 'x', 'z'))


def block_shape(rows, width, axes):
    lead = tuple(SIZE[a] for a in 'zy' if a in axes)
    if width is None:
        return (((SIZE['x'],) if 'x' in axes else ()) + lead + (rows, 512))
    return lead + (rows, width * (SIZE['x'] if 'x' in axes else 1))


def reduce_shapes():
    shapes = []
    for name, colour, rows, width in REDUCED:
        first, middle, last = ORDERS[colour]
        whole = block_shape(rows, width, 'xzy')
        one = [whole, whole]
        rest = middle + last
        for which in (0, 1):
            for step in range(SIZE[first] // 2):
                shape = list(block_shape(rows, width, rest))
                if step == 0:
                    axis = HALF[first]
                    at = [a for a in ('x' if width is None else '') + 'zy' if a in rest].index(axis)
                    shape[at] //= 2
                one.append(tuple(shape))
        one.append((SIZE[middle] - 1,) + block_shape(rows, width, last))
        one.append((SIZE[last] - 1,) + block_shape(rows, width, ''))
        shapes.append(one)
    return shapes


def reduce_kernel(*refs):
    n = len(REDUCED)
    grads, (small_g, head_g) = refs[:n], refs[n:n + 2]
    pieces, (small_o, head_o) = refs[n + 2:2 * n + 2], refs[2 * n + 2:2 * n + 4]
    scratch = list(refs[2 * n + 4:])
    tensors = []
    for (name, colour, rows, width), grad, shapes in zip(REDUCED, grads, reduce_shapes()):
        bufs = [scratch.pop(0) for _ in shapes]
        steps = SIZE[ORDERS[colour][0]] // 2
        tensors.append(dict(rows='zy', width=width, grad=grad, sum=bufs[0], peer=bufs[1], colour=colour,
                            ring=(bufs[2:2 + steps], bufs[2 + steps:2 + 2 * steps]), slots=bufs[-2:]))
    small, small_peer, small_y, small_z, small_x, head, head_c, head_y, head_z, last, send_sems, recv_sems, load_sems, out_sems = scratch
    net = Net(send_sems, recv_sems)
    me = net.me
    net.barrier()
    c = me['c']
    red = [Reduce(net, [t for t in tensors if t['colour'] == k], *ORDERS[k], load_sems.at[k]) for k in range(3)]
    a, b, d = red
    loads = [pltpu.make_async_copy(small_g.at[:, :, c], small, out_sems.at[0]), pltpu.make_async_copy(head_g, head.at[0], out_sems.at[1])]
    for copy in loads:
        copy.start()
    tiny = [net.send(small_g.at[:, :, 1 - c], small_peer, 'c', 1), net.send(head_g, head_c, 'c', 1)]
    for i in range(4):
        for r in red:
            if i < len(r.targets()):
                r.start(i)
        if i > 0:
            a.start(3 + i)
    a.start(7)
    for r in red:
        r.ring(1)
    for copy in loads:
        copy.wait()
    for copy in tiny:
        copy.wait_recv()
    accumulate(small, [small_peer])
    head[0] = head[0] + head_c[...]
    a.ring(2)
    tiny = [net.send(small.at[:, net.at('y', i)], small_y.at[i - 1], 'y', i) for i in (1, 2, 3)]
    tiny += [net.send(head.at[0], head_y.at[i - 1], 'y', i) for i in (1, 2, 3)]
    b.ring(2)
    d.ring(2)
    a.ring(3)
    for copy in tiny:
        copy.wait_recv()
    accumulate(small.at[:, me['y']], [small_y.at[i] for i in range(3)])
    head[1] = head[0] + head_y[0] + head_y[1] + head_y[2]
    a.ring(4)
    tiny = [net.send(small.at[net.at('z', i), me['y']], small_z.at[i - 1], 'z', i) for i in range(1, 8)]
    tiny += [net.send(head.at[1], head_z.at[i - 1], 'z', i) for i in range(1, 8)]
    b.ring(3)
    b.direct(1)
    d.ring(3)
    d.direct(1)
    for copy in tiny:
        copy.wait_recv()
    mine = small[me['z'], me['y']]
    total = head[1]
    for i in range(7):
        mine = mine + small_z[i]
        total = total + head_z[i]
    small_x[3, 0:8] = mine
    small_x[3, 8:16] = total
    a.ring(5)
    a.direct(1)
    tiny = [net.send(small_x.at[3], small_x.at[i - 1], 'x', i) for i in (1, 2, 3)]
    d.direct_done(1)
    d.direct(2)
    a.direct_done(1)
    a.direct(2)
    b.direct_done(1)
    b.direct(2)
    for copy in tiny:
        copy.wait_recv()
    whole = small_x[0] + small_x[1] + small_x[2] + small_x[3]
    last[...] = whole
    outs = [pltpu.make_async_copy(last.at[0:8], small_o, out_sems.at[0]), pltpu.make_async_copy(last.at[8:16], head_o, out_sems.at[1])]
    for r in (d, a, b):
        r.direct_done(2)
    for i, (t, piece) in enumerate(zip(tensors, pieces)):
        outs.append(pltpu.make_async_copy(part(t, t['sum'], x=me['x'], y=me['y'], z=me['z']), piece, out_sems.at[2 + i]))
    for copy in outs:
        copy.start()
    net.finish()
    for copy in outs:
        copy.wait()


def reduce_all(grads, small, head):
    f32 = jnp.float32
    hbm = pl.BlockSpec(memory_space=pl.ANY)
    outs = [(rows, 512 if width is None else width) for _, _, rows, width in REDUCED] + [(8, 128), (8, 128)]
    bufs = [shape for one in reduce_shapes() for shape in one]
    bufs += [(8, 4, 8, 128), (8, 4, 8, 128), (3, 8, 8, 128), (7, 8, 128), (4, 16, 128), (2, 8, 128), (8, 128), (3, 8, 128), (7, 8, 128), (16, 128)]
    return pl.pallas_call(
        reduce_kernel, out_shape=[jax.ShapeDtypeStruct(s, f32) for s in outs], in_specs=[hbm] * 8, out_specs=[hbm] * 8,
        scratch_shapes=[pltpu.VMEM(s, f32) for s in bufs] + [pltpu.SemaphoreType.DMA((200,)), pltpu.SemaphoreType.DMA((200,)),
                        pltpu.SemaphoreType.DMA((3, 16)), pltpu.SemaphoreType.DMA((8,))],
        compiler_params=pltpu.CompilerParams(collective_id=1, has_side_effects=True, vmem_limit_bytes=62 << 20),
        name='reduce_gradients')(*grads, small, head)


EPS = 1e-6
BF = jnp.bfloat16
VECTORS = 13
PER_X = 42


def product(form, left, right):
    return jnp.einsum(form, left, right, preferred_element_type=jnp.float32)


def norm_forward(values, gain, shift):
    width = values.shape[-1]
    mean_val = jnp.sum(values, axis=-1, keepdims=True) / width
    square = jnp.sum(values * values, axis=-1, keepdims=True) / width
    inv_std = lax.rsqrt(jnp.maximum(square - mean_val * mean_val, 0.0) + EPS)
    standard = (values - mean_val) * inv_std
    return standard * gain + shift, standard, inv_std


def norm_backward(grad_out, gain, standard, inv_std):
    width = grad_out.shape[-1]
    grad_std = grad_out * gain
    first = jnp.sum(grad_std, axis=-1, keepdims=True) / width
    second = jnp.sum(grad_std * standard, axis=-1, keepdims=True) / width
    return inv_std * (grad_std - first - standard * second)


def gelu_grad(pre_act, grad_out):
    return jax.vjp(jax.nn.gelu, pre_act)[1](grad_out)[0]


def lead_sum(values):
    return jnp.sum(values.reshape(-1, values.shape[-1]), axis=0)


def pack_small(x, b_stem, ln1_g, ln1_b, ln2_g, ln2_b, b_ch2, lnf_g, lnf_b, b_ch1, w_tok1, w_tok2, b_tok1, b_head):
    vec = jnp.concatenate([b_stem[None], ln1_g, ln1_b, ln2_g, ln2_b, b_ch2, lnf_g[None], lnf_b[None]], axis=0).reshape(-1)
    vec = jnp.concatenate([vec, b_ch1.reshape(-1)])
    spread = lax.dynamic_update_slice(jnp.zeros((4 * PER_X,), jnp.float32), vec, (x * PER_X,))
    tok = jnp.concatenate([w_tok1.reshape(-1), w_tok2.reshape(-1), b_tok1.reshape(-1)])
    tok = jnp.where(x == 0, tok.astype(jnp.float32), 0.0)
    first = jnp.concatenate([spread, tok, jnp.zeros((1024 - 4 * PER_X - tok.shape[0],), jnp.float32)])
    head = lax.dynamic_update_slice(jnp.zeros((1024,), jnp.float32), b_head, (x * 256,))
    return jnp.concatenate([first, head]).reshape(16, 128)


def solution(mesh):
    def step(patches, labels, w_stem, b_stem, ln1_g, ln1_b, w_tok1, b_tok1, w_tok2,
             ln2_g, ln2_b, w_ch1, b_ch1, w_ch2, b_ch2, lnf_g, lnf_b, w_head, b_head):
        x = lax.axis_index('tp')
        images = patches.shape[0] // 4
        total = 4096.0
        small_p = pack_small(x, b_stem, ln1_g, ln1_b, ln2_g, ln2_b, b_ch2, lnf_g, lnf_b, b_ch1,
                             w_tok1.astype(BF), w_tok2.astype(BF), b_tok1, b_head)
        head_p = jnp.pad(w_head.astype(BF), ((0, 0), (0, 6)))
        stem, head, c10, c11, c20, c21, small, bias = gather_all(w_stem.astype(BF), head_p, w_ch1.astype(BF), w_ch2.astype(BF), small_p)
        stem, head = stem.reshape(3072, 512), head.reshape(512, 1024)
        ch1 = [c10.reshape(512, 2048), c11.reshape(512, 2048)]
        ch2 = [c20.reshape(2048, 512), c21.reshape(2048, 512)]
        small = small.reshape(64, 1024)
        vec = small[:, :4 * PER_X].reshape(64, 4, PER_X)
        chan = vec[:, :, :26].reshape(64, 4, VECTORS, 2).transpose(2, 1, 0, 3).reshape(VECTORS, 512)
        stem_b, lnf_gf, lnf_bf = chan[0], chan[11], chan[12]
        ln1_gf, ln1_bf, ln2_gf, ln2_bf, ch2_b = (chan[1 + 2 * i:3 + 2 * i] for i in range(5))
        ch1_b = vec[:, :, 26:].reshape(64, 4, 2, 8).transpose(2, 1, 0, 3).reshape(2, 2048)
        base = 4 * PER_X
        tok1 = small[:, base:base + 392].reshape(64, 2, 49, 4).transpose(1, 2, 0, 3).reshape(2, 49, 256).astype(BF)
        tok2 = small[:, base + 392:base + 784].reshape(64, 2, 4, 49).transpose(1, 0, 2, 3).reshape(2, 256, 49).astype(BF)
        tok_b = small[:, base + 784:base + 792].reshape(64, 2, 4).transpose(1, 0, 2).reshape(2, 256)
        head_b = bias.reshape(1024)

        mine = lax.dynamic_slice_in_dim(patches, x * images, images, 0)
        label = lax.dynamic_slice_in_dim(labels, x * images, images, 0)
        tokens = patches.shape[1]
        resid = product('bsp,pc->bsc', mine, stem) + stem_b
        saved = []
        for layer in range(2):
            n1, s1, i1 = norm_forward(resid, ln1_gf[layer], ln1_bf[layer])
            n1 = n1.astype(BF)
            tok_pre = product('bsc,sj->bcj', n1, tok1[layer]) + tok_b[layer]
            tok_act = jax.nn.gelu(tok_pre).astype(BF)
            resid = resid + product('bcj,js->bsc', tok_act, tok2[layer])
            n2, s2, i2 = norm_forward(resid, ln2_gf[layer], ln2_bf[layer])
            n2 = n2.astype(BF)
            ch_pre = product('bsc,cd->bsd', n2, ch1[layer]) + ch1_b[layer]
            ch_act = jax.nn.gelu(ch_pre).astype(BF)
            resid = resid + product('bsd,dc->bsc', ch_act, ch2[layer]) + ch2_b[layer]
            saved.append((n1, s1, i1, tok_pre, tok_act, n2, s2, i2, ch_pre, ch_act))
        pooled = jnp.mean(resid, axis=1)
        head_in, head_std, head_inv = norm_forward(pooled, lnf_gf, lnf_bf)
        head_in = head_in.astype(BF)
        column = jnp.arange(1024)
        valid = (column % 256) < 250
        class_id = jnp.where(valid, (column // 256) * 250 + column % 256, -1)
        logits = jnp.where(valid, product('bc,ck->bk', head_in, head) + head_b, -jnp.inf)
        is_label = class_id[None, :] == label[:, None]
        row_max = jnp.max(logits, axis=1)
        shifted = jnp.exp(logits - row_max[:, None])
        class_sum = jnp.sum(shifted, axis=1)
        picked = jnp.sum(jnp.where(is_label, logits, 0.0), axis=1)
        loss = jnp.sum(row_max + jnp.log(class_sum) - picked) / total
        d_logits = (shifted / class_sum[:, None] - is_label.astype(jnp.float32)) / total
        d_logits_bf = d_logits.astype(BF)
        g_head = product('bc,bk->ck', head_in, d_logits_bf)
        g_bias = jnp.where(column == 250, loss, jnp.sum(d_logits, axis=0))
        d_head = product('bk,ck->bc', d_logits_bf, head)
        g_lnf_g, g_lnf_b = jnp.sum(d_head * head_std, axis=0), jnp.sum(d_head, axis=0)
        d_pooled = norm_backward(d_head, lnf_gf, head_std, head_inv)
        d_resid = jnp.broadcast_to((d_pooled / tokens)[:, None, :], resid.shape)
        grad = {}
        for layer in (1, 0):
            n1, s1, i1, tok_pre, tok_act, n2, s2, i2, ch_pre, ch_act = saved[layer]
            grad['b_ch2', layer] = lead_sum(d_resid)
            d_bf = d_resid.astype(BF)
            grad['w_ch2', layer] = product('bsd,bsc->dc', ch_act, d_bf)
            d_pre = gelu_grad(ch_pre, product('bsc,dc->bsd', d_bf, ch2[layer]))
            grad['b_ch1', layer] = lead_sum(d_pre)
            d_pre = d_pre.astype(BF)
            grad['w_ch1', layer] = product('bsc,bsd->cd', n2, d_pre)
            d_n2 = product('bsd,cd->bsc', d_pre, ch1[layer])
            grad['ln2_g', layer], grad['ln2_b', layer] = lead_sum(d_n2 * s2), lead_sum(d_n2)
            d_mid = d_resid + norm_backward(d_n2, ln2_gf[layer], s2, i2)
            d_bf = d_mid.astype(BF)
            grad['w_tok2', layer] = product('bcj,bsc->js', tok_act, d_bf)
            d_tok = gelu_grad(tok_pre, product('bsc,js->bcj', d_bf, tok2[layer]))
            grad['b_tok1', layer] = lead_sum(d_tok)
            d_tok = d_tok.astype(BF)
            grad['w_tok1', layer] = product('bsc,bcj->sj', n1, d_tok)
            d_n1 = product('bcj,sj->bsc', d_tok, tok1[layer])
            grad['ln1_g', layer], grad['ln1_b', layer] = lead_sum(d_n1 * s1), lead_sum(d_n1)
            d_resid = d_mid + norm_backward(d_n1, ln1_gf[layer], s1, i1)
        g_b_stem = lead_sum(d_resid)
        g_stem = product('bsp,bsc->pc', mine, d_resid.astype(BF))

        def both(name):
            return [grad[name, 0], grad[name, 1]]

        chan = jnp.stack([g_b_stem] + both('ln1_g') + both('ln1_b') + both('ln2_g') + both('ln2_b') + both('b_ch2') + [g_lnf_g, g_lnf_b])
        vec = jnp.concatenate([chan.reshape(VECTORS, 4, 64, 2).transpose(2, 1, 0, 3).reshape(64, 4, 26),
                               jnp.stack(both('b_ch1')).reshape(2, 4, 64, 8).transpose(2, 1, 0, 3).reshape(64, 4, 16)], axis=2)
        tok = [jnp.stack(both('w_tok1')).reshape(2, 49, 64, 4).transpose(2, 0, 1, 3).reshape(64, 392),
               jnp.stack(both('w_tok2')).reshape(2, 64, 4, 49).transpose(1, 0, 2, 3).reshape(64, 392),
               jnp.stack(both('b_tok1')).reshape(2, 64, 4).transpose(1, 0, 2).reshape(64, 8)]
        small_g = jnp.concatenate([vec.reshape(64, 168)] + tok + [jnp.zeros((64, 64), jnp.float32)], axis=1)
        rows = (8, 4, 2, 8)
        grads = [g_stem.reshape(8, 4, 2, 48, 512), g_head.reshape(rows + (1024,)),
                 grad['w_ch1', 0].reshape(rows + (2048,)), grad['w_ch2', 0].reshape((4,) + rows + (512,)),
                 grad['w_ch1', 1].reshape(rows + (2048,)), grad['w_ch2', 1].reshape((4,) + rows + (512,))]
        o = reduce_all(grads, small_g.reshape(8, 4, 2, 8, 128), g_bias.reshape(8, 128))
        g_stem, g_head, c10, c20, c11, c21, small, bias = o
        small, bias = small.reshape(1024), bias.reshape(1024)
        vec = lax.dynamic_slice(small, (x * PER_X,), (PER_X,))
        chan = vec[:26].reshape(VECTORS, 2)
        pair = [chan[1 + 2 * i:3 + 2 * i] for i in range(5)]
        tok = small[base:]
        return (bias[250], g_stem, chan[0], pair[0], pair[1], tok[:392].reshape(2, 49, 4), tok[784:792].reshape(2, 4),
                tok[392:784].reshape(2, 4, 49), pair[2], pair[3], jnp.stack([c10, c11]), vec[26:].reshape(2, 8), jnp.stack([c20, c21]),
                pair[4], chan[11], chan[12], g_head[:, :250], lax.dynamic_slice(bias, (x * 256,), (250,)))

    vec_spec, layer_vec = P(('tp', 'fsdp')), P(None, ('tp', 'fsdp'))
    specs = (P('fsdp', 'tp'), vec_spec, layer_vec, layer_vec, P(None, None, 'fsdp'), P(None, 'fsdp'),
             P(None, 'fsdp', None), layer_vec, layer_vec, P(None, 'fsdp', 'tp'), layer_vec,
             P(None, ('tp', 'fsdp'), None), layer_vec, vec_spec, vec_spec, P('fsdp', 'tp'), P('tp'))
    return jax.shard_map(step, mesh=mesh, in_specs=(P('fsdp', None, None), P('fsdp')) + specs,
                         out_specs=(P(),) + specs, check_vma=False)
```
